128 devices in a mesh: row: 2 (over z_lo), col: 64 (over y, x, z_hi, core).
Axes of the slice: x: 4, y: 4, z: 4 (z_hi: 2, z_lo: 2; z = z_hi * 2 + z_lo), core: 2. Of those that a mesh axis runs over, the one named last changes fastest.
Arguments:
- tokens: bfloat16 [512, 4608], P('col', 'row'), may hold values from -6 to 6
- pre_gain: float32 [2, 4608], P(None, 'row'), may hold values from -0.6 to 0.6
- post_gain: float32 [2, 4608], P(None, 'row'), may hold values from -0.6 to 0.6
- gate_weight: bfloat16 [2, 4608, 36864], P(None, ('row', 'col')), may hold values from -0.09375 to 0.09375
- up_weight: bfloat16 [2, 4608, 36864], P(None, ('row', 'col')), may hold values from -0.09375 to 0.09375
- down_weight: bfloat16 [2, 36864, 4608], P(None, ('row', 'col')), may hold values from -0.13541667 to 0.13541667
Outputs:
- stream: bfloat16 [512, 4608], P('col', 'row')
The draws below stay inside these ranges and needn't reach their ends.
All inputs are finite; a program needn't handle non-finite values.
Results may differ from the reference program's by a relative error of at most 0.019.
Values may be sent and summed in bfloat16 or wider, within the bound.
A program may use at most 128 MiB of HBM per device.

```python
import math
import jax
import jax.numpy as jnp
from jax import lax

D = 4608
FF = 36864
LAYERS = 2
TOKENS = 512


def draw_down_weight(key, part):
    key_main = jax.random.fold_in(key, 11)
    key_rough = jax.random.fold_in(key, 12)
    entries = jax.random.truncated_normal(key_main, -6.0, 6.0, (LAYERS, FF, D), jnp.float32)
    low_end = 0.5
    high_end = 2.0
    ramp = jnp.linspace(math.log(low_end), math.log(high_end), D, dtype=jnp.float32)
    rough = jax.random.uniform(key_rough, (LAYERS, 1, D), jnp.float32, math.log(0.7), math.log(1.4))
    scales = jnp.exp(ramp[None, None, :] + rough)
    return (entries * scales * FF ** (-0.5)).astype(jnp.bfloat16)


def block_levels(own_key, shape, shards, least, top_value):
    loudness = 1.0
    for axis_at, blocks in shards:
        draws = jax.random.uniform(jax.random.fold_in(jax.random.fold_in(own_key, 6), axis_at), (blocks,), jnp.float32, least / len(shards), top_value / len(shards))
        loudness = loudness * jnp.repeat(jnp.exp(draws), shape[axis_at] // blocks).reshape((-1,) + (1,) * (len(shape) - 1 - axis_at))
    return loudness


def bell_draw(stream_key, extent, scale, most, pieces=(), held_as=jnp.bfloat16):
    drawn = jax.random.normal(stream_key, extent, jnp.float32) * scale
    if len(pieces) > 0:
        drawn = block_levels(stream_key, extent, pieces, -0.22, 0.18) * drawn
    return jnp.clip(drawn, min=-most, max=most).astype(held_as)


def setup_inputs(seed: int = 0) -> dict:
    seeds = jax.random.split(jax.random.key(seed), 7)
    return {
        "tokens": bell_draw(seeds[0], (TOKENS, D), 1.0, 6.0, ((0, 64), (1, 2))),
        "pre_gain": jnp.clip(jax.random.uniform(seeds[1], (LAYERS, D), jnp.float32, -0.6, 0.6) * block_levels(seeds[1], (LAYERS, D), ((1, 2),), -0.4, 0.0), -0.6, 0.6),
        "post_gain": jnp.clip(jax.random.uniform(seeds[2], (LAYERS, D), jnp.float32, -0.6, 0.6) * block_levels(seeds[2], (LAYERS, D), ((1, 2),), -0.4, 0.0), -0.6, 0.6),
        "gate_weight": bell_draw(seeds[3], (LAYERS, D, FF), D ** -0.5, 0.09375, ((1, 128),)),
        "up_weight": bell_draw(seeds[4], (LAYERS, D, FF), D ** -0.5, 0.09375, ((1, 128),)),
        "down_weight": draw_down_weight(jax.random.fold_in(seeds[6], 71), 0),
    }


norm_eps = 1e-06

def reference(tokens, pre_gain, post_gain, gate_weight, up_weight, down_weight):
    current = tokens
    for layer_index in range(LAYERS):
        values = current.astype(jnp.float32)
        mean_sq = lax.optimization_barrier(jnp.mean(values * values, axis=1, keepdims=True))
        normed = (values * lax.rsqrt(mean_sq + norm_eps) * (1.0 + pre_gain[layer_index])[None, :]).astype(jnp.bfloat16)
        gate = jnp.dot(normed, gate_weight[layer_index], preferred_element_type=jnp.float32)
        up_proj = jnp.dot(normed, up_weight[layer_index], preferred_element_type=jnp.float32)
        hidden = (jax.nn.gelu(gate, approximate=True) * up_proj).astype(jnp.bfloat16)
        branch = jnp.dot(hidden, down_weight[layer_index], preferred_element_type=jnp.float32)
        branch_sq = lax.optimization_barrier(jnp.mean(branch * branch, axis=1, keepdims=True))
        post = branch * lax.rsqrt(branch_sq + norm_eps) * (1.0 + post_gain[layer_index])[None, :]
        current = (values + post).astype(jnp.bfloat16)
    return current
```

```python
import functools
import math

import jax
import jax.numpy as jnp
from jax import lax
from jax.experimental import pallas as pl
from jax.experimental.pallas import tpu as pltpu
from jax.sharding import PartitionSpec as P

MESH = pl.DeviceIdType.MESH
EPS = 1e-06
D, FF, LAYERS, TOKENS = 4608, 36864, 2, 512
HALF = D // 2
THIRD = HALF // 3
ROWS = 36
SOURCES = 64
WIDE, NARROW = 640, 512
GROUP = WIDE + NARROW
PARTS = 2
PART = SOURCES // PARTS
STORED = 288
SPARE = 64
ORDER = (("z", "x", "y"), ("x", "y", "z"), ("y", "z", "x"))
F32, BF16 = jnp.float32, jnp.bfloat16


def slab_shape(d, full):
    z = 1 if d == "z" or "z" not in full else 2
    y = 1 if d == "y" or "y" not in full else 4
    x = 1 if d == "x" or "x" not in full else 4
    return (z, y, x, z)


def kernel(
    tok, pre, post, gate, up, down, out,
    wbuf, dbuf, xbuf, rbuf, acc, xcat, tile, hid, nbuf, psend, precv, ssend, srecv, branch, cur,
    *rest,
):
    rs_in = [[rest[t * 3 + i] for i in range(3)] for t in range(3)]
    (w_send, w_recv, d_send, d_recv, a0_send, a0_recv, ag_send, ag_recv, rs_send, rs_recv,
     p_send, p_recv, s_send, s_recv) = rest[9:]
    r = lax.axis_index("row")
    c = lax.axis_index("col")
    y, x, zh, core = c // 16, (c // 4) % 4, (c // 2) % 2, c % 2
    own = {"y": y, "x": x, "z": r * 2 + zh}
    wide = (zh + x + y) % 2 == 0

    def device(ty, tx, tz, tcore):
        return (tz // 2, ty * 16 + tx * 4 + (tz % 2) * 2 + tcore)

    def remote(src, dst, send, recv, where):
        return pltpu.make_async_remote_copy(
            src_ref=src, dst_ref=dst, send_sem=send, recv_sem=recv, device_id=where, device_id_type=MESH
        )

    def weight_start(tz, ty, tx, k, layer):
        tzl, tzh = tz // 2, tz % 2
        group = tzl * 16 + ty * 4 + tx
        twide = (tzh + tx + ty) % 2 == 0
        where = device(ty, tx, tz, r)
        me = (k == 0) & (core == r)
        for is_wide, width in ((True, WIDE), (False, NARROW)):
            start = group * GROUP + tzh * (NARROW if is_wide else WIDE)
            for m, ref in enumerate((gate, up)):
                src = ref.at[layer, :, pl.ds(pl.multiple_of(start, 128), width)]
                dst = wbuf.at[layer, m, c, :, pl.ds(0, width)]
                right = twide if is_wide else jnp.logical_not(twide)

                @pl.when(right & me)
                def _():
                    pltpu.make_async_copy(src, dst, w_recv.at[layer, y // 2]).start()

                @pl.when(right & jnp.logical_not(me))
                def _():
                    remote(src, dst, w_send.at[0], w_recv.at[layer, y // 2], where).start()

    def weights_start(layer, lo, hi):
        def body(k, carry):
            dz, dx, dy = k % 4, (k // 4) % 4, k // 16
            weight_start((own["z"] + dz) % 4, (y + dy) % 4, (x + dx) % 4, k, layer)
            return carry

        lax.fori_loop(lo, hi, body, 0)

    def weights_wait(layer, part):
        for is_wide, width in ((True, WIDE), (False, NARROW)):
            ref = wbuf.at[layer, :, pl.ds(part * PART, PART), :, pl.ds(0, width)]

            @pl.when(wide if is_wide else jnp.logical_not(wide))
            def _():
                pltpu.make_async_copy(ref, ref, w_recv.at[layer, part]).wait()

    def weights_sent():
        mine = core == r
        for is_wide in (True, False):
            right = wide if is_wide else jnp.logical_not(wide)

            def take(n_wide, n_narrow):
                big = wbuf.at[:, :, pl.ds(0, n_wide), :, pl.ds(0, WIDE)]
                small = wbuf.at[:, :, pl.ds(0, n_narrow), :, pl.ds(0, NARROW)]
                pltpu.make_async_copy(big, big, w_send.at[0]).wait()
                pltpu.make_async_copy(small, small, w_send.at[0]).wait()

            @pl.when(right & mine)
            def _():
                take(31 if is_wide else 32, 32 if is_wide else 31)

        @pl.when(jnp.logical_not(mine))
        def _():
            big = wbuf.at[:, :, pl.ds(0, 32), :, pl.ds(0, WIDE)]
            small = wbuf.at[:, :, pl.ds(0, 32), :, pl.ds(0, NARROW)]
            pltpu.make_async_copy(big, big, w_send.at[0]).wait()
            pltpu.make_async_copy(small, small, w_send.at[0]).wait()

    partner = (r, c + 1 - 2 * core)

    def down_each(case):
        for h in range(2):
            for k in range(2):
                here = (zh == h) & (core == k)
                start = 0 if h == 0 else NARROW
                case(here & wide, 0, STORED, h * 576 + k * STORED - start)
                start = 0 if h == 0 else WIDE
                if h == k:
                    case(here & jnp.logical_not(wide), 0, STORED, h * 576 + k * STORED - start)
                else:
                    first = 0 if h == 0 else SPARE
                    case(
                        here & jnp.logical_not(wide), first, STORED - SPARE,
                        h * 576 + k * STORED + first - start,
                    )

    def down_start():
        for layer in range(LAYERS):
            def case(condition, first, rows, to):
                src = down.at[layer, pl.ds(first, rows)]
                dst = dbuf.at[layer, pl.ds(to, rows)]

                @pl.when(condition)
                def _():
                    pltpu.make_async_copy(src, dst, d_recv.at[layer]).start()
                    remote(src, dst, d_send.at[0], d_recv.at[layer], partner).start()

            down_each(case)
            for h in range(2):
                giver = (zh == h) & (core == 1 - h) & jnp.logical_not(wide)
                src = down.at[layer, pl.ds(STORED - SPARE if h == 0 else 0, SPARE)]
                dst = dbuf.at[layer, pl.ds(0 if h == 0 else 576, SPARE)]

                @pl.when(giver)
                def _():
                    for k in range(2):
                        remote(
                            src, dst, d_send.at[0], d_recv.at[layer], (r, y * 16 + x * 4 + (1 - h) * 2 + k)
                        ).start()

    def down_wait(layer):
        for is_wide, width in ((True, WIDE), (False, NARROW)):
            ref = dbuf.at[layer, pl.ds(0, width)]

            @pl.when(wide if is_wide else jnp.logical_not(wide))
            def _():
                pltpu.make_async_copy(ref, ref, d_recv.at[layer]).wait()

    def down_sent():
        full = wide | (zh == core)

        @pl.when(full)
        def _():
            ref = dbuf.at[:, pl.ds(0, STORED)]
            pltpu.make_async_copy(ref, ref, d_send.at[0]).wait()

        @pl.when(jnp.logical_not(full))
        def _():
            ref = dbuf.at[:, pl.ds(0, STORED + SPARE)]
            pltpu.make_async_copy(ref, ref, d_send.at[0]).wait()

    def slots(buf, layer, third, at):
        def pick(v, n):
            return pl.ds(0, n) if v is None else pl.ds(v, 1)

        z = at["z"]
        return buf.at[
            layer, third,
            pick(None if z is None else z // 2, 2),
            pick(at["y"], 4),
            pick(at["x"], 4),
            pick(None if z is None else z % 2, 2),
        ]

    def target(d, k):
        where = {**own, d: (own[d] + k) % 4}
        return where, device(where["y"], where["x"], where["z"], core)

    def gather_copy(layer, third, i, k, incoming):
        d = ORDER[third][i]
        at = {e: (None if e in ORDER[third][:i] else own[e]) for e in "xyz"}
        _, where = target(d, k)
        if incoming:
            at[d] = (own[d] + 4 - k) % 4
        ref = slots(xbuf, layer, third, at)
        return remote(ref, ref, ag_send.at[layer, third, i, k - 1], ag_recv.at[layer, third, i, k - 1], where)

    def scatter_copy(layer, third, i, k, incoming):
        order = ORDER[third][::-1]
        d = order[i]
        at = {e: (None if e in order[i + 1:] else own[e]) for e in "xyz"}
        there, where = target(d, k)
        at[d] = there[d]
        dst = rs_in[third][i].at[layer, k - 1]
        src = dst if incoming else slots(rbuf, layer, third, at)
        return remote(src, dst, rs_send.at[layer, third, i, k - 1], rs_recv.at[layer, third, i, k - 1], where)

    def scatter_add(layer, third, i):
        order = ORDER[third][::-1]
        free = order[i + 1:]
        sizes = [4 for _ in free]
        count = math.prod(sizes) if sizes else 1
        buf = rs_in[third][i]

        def body(n, carry):
            at, inner = dict(own), {"z": 0, "y": 0, "x": 0}
            for e in free:
                at[e] = n % 4
                inner[e] = n % 4
                n = n // 4
            total = rbuf[layer, third, at["z"] // 2, at["y"], at["x"], at["z"] % 2].astype(F32)
            for k in range(3):
                total += buf[layer, k, inner["z"] // 2, inner["y"], inner["x"], inner["z"] % 2].astype(F32)
            if i < 2:
                rbuf[layer, third, at["z"] // 2, at["y"], at["x"], at["z"] % 2] = total.astype(BF16)
            else:
                branch[:, third * THIRD:(third + 1) * THIRD] = total
            return carry

        if count == 1:
            body(0, 0)
        else:
            lax.fori_loop(0, count, body, 0)

    def pair_sum(value, n):
        part = jnp.sum(value * value, axis=1, keepdims=True)
        ssend[n] = jnp.broadcast_to(part, (8, 128))
        copy = remote(ssend.at[n], srecv.at[n], s_send.at[n], s_recv.at[n], (1 - r, c))
        copy.start()
        copy.wait()
        return part + srecv[n][:, 0:1]

    def norm_in(layer):
        values = cur[...]
        scale = lax.rsqrt(pair_sum(values, 2 * layer) / D + EPS)
        normed = values * scale * (1.0 + pre[layer:layer + 1, :])
        for t in range(3):
            nbuf[layer, t] = normed[:, t * THIRD:(t + 1) * THIRD].astype(BF16)

    def home_copy(layer):
        home = (core + r) % 2
        where = (home, y * 16 + x * 4 + zh * 2 + r)
        return nbuf.at[layer], xbuf.at[layer, :, home, y, x, zh], where

    def home_start(layer):
        src, dst, where = home_copy(layer)
        me = (core == 0) & (r == 0)

        @pl.when(me)
        def _():
            pltpu.make_async_copy(src, dst, a0_recv.at[layer]).start()

        @pl.when(jnp.logical_not(me))
        def _():
            remote(src, dst, a0_send.at[layer], a0_recv.at[layer], where).start()

    def home_wait(layer):
        ref = xbuf.at[layer, :, r, y, x, zh]
        pltpu.make_async_copy(ref, ref, a0_recv.at[layer]).wait()

    def home_sent(layer):
        @pl.when(jnp.logical_not((core == 0) & (r == 0)))
        def _():
            ref = nbuf.at[layer]
            pltpu.make_async_copy(ref, ref, a0_send.at[layer]).wait()

    def gather(layer, between):
        home_start(layer)
        between(0)
        home_wait(layer)
        for i in range(3):
            for t in range(3):
                for k in (1, 3, 2):
                    gather_copy(layer, t, i, k, False).start()
            between(i + 1)
            for t in range(3):
                for k in (1, 3, 2):
                    gather_copy(layer, t, i, k, True).wait_recv()

    def spread(layer):
        for t in range(3):
            def put(n, carry):
                piece = xbuf[layer, t, n // 4, n % 4]
                rows = piece.astype(F32).reshape(64, THIRD).astype(BF16)
                xcat[pl.ds(pl.multiple_of(n * 64, 64), 64), t * THIRD:(t + 1) * THIRD] = rows
                return carry

            lax.fori_loop(0, 8, put, 0)

    def project(layer):
        def pack(part, n, carry):
            for m in range(2):
                blocks = [wbuf[layer, m, part * PART + n * 4 + s].astype(F32) for s in range(4)]
                rows = pl.ds(pl.multiple_of(n * 4 * ROWS, 16), 4 * ROWS)
                tile[m, rows] = jnp.concatenate(blocks, axis=0).astype(BF16)
            return carry

        def multiply(part, n, carry):
            rows = pl.ds(pl.multiple_of(n * 128, 128), 128)
            lanes = slice(part * PART * ROWS, (part + 1) * PART * ROWS)
            for m in range(2):
                value = jnp.dot(xcat[rows, lanes], tile[m], preferred_element_type=F32)
                if part > 0:
                    value += acc[m, rows]
                acc[m, rows] = value
            return carry

        for part in range(PARTS):
            weights_wait(layer, part)
            lax.fori_loop(0, PART // 4, functools.partial(pack, part), 0)
            lax.fori_loop(0, 4, functools.partial(multiply, part), 0)

    def activate(layer):
        for m in range(2):
            psend[layer, m] = acc[m, 256:512].astype(BF16)
        copy = remote(psend.at[layer], precv.at[layer], p_send.at[layer], p_recv.at[layer], partner)
        copy.start()
        copy.wait()
        g = acc[0, 0:256] + precv[layer, 0].astype(F32)
        u = acc[1, 0:256] + precv[layer, 1].astype(F32)
        column = lax.broadcasted_iota(jnp.int32, (256, WIDE), 1)
        live = wide | (column < NARROW)
        hidden = jnp.where(live, jax.nn.gelu(g, approximate=True) * u, 0.0)
        hid[...] = hidden.astype(BF16)

    def project_down(layer):
        down_wait(layer)
        for t in range(3):
            for half in range(2):
                lanes = slice(half * HALF + t * THIRD, half * HALF + (t + 1) * THIRD)
                part = jnp.dot(hid[...], dbuf[layer, :, lanes], preferred_element_type=F32)
                rbuf[layer, t, half] = part.reshape(4, 4, 2, 8, THIRD).astype(BF16)
            for k in (1, 3, 2):
                scatter_copy(layer, t, 0, k, False).start()

    def scatter(layer):
        for i in range(3):
            for t in range(3):
                for k in (1, 3, 2):
                    scatter_copy(layer, t, i, k, True).wait_recv()
                scatter_add(layer, t, i)
                if i < 2:
                    for k in (1, 3, 2):
                        scatter_copy(layer, t, i + 1, k, False).start()

    def norm_out(layer):
        total = branch[...]
        scale = lax.rsqrt(pair_sum(total, 2 * layer + 1) / D + EPS)
        post_norm = total * scale * (1.0 + post[layer:layer + 1, :])
        result = (cur[...] + post_norm).astype(BF16)
        if layer == LAYERS - 1:
            out[...] = result
        else:
            cur[...] = result.astype(F32)

    @pl.when(jnp.logical_not(wide))
    def _():
        dbuf[:, NARROW:WIDE] = jnp.zeros((LAYERS, WIDE - NARROW, D), BF16)

    cur[...] = tok[...].astype(F32)
    norm_in(0)
    gather(0, lambda n: weights_start(0, n * 16, n * 16 + 16))
    down_start()
    weights_start(1, 0, 64)
    for layer in range(LAYERS):
        if layer > 0:
            norm_in(layer)
            gather(layer, lambda n: None)
        spread(layer)
        project(layer)
        activate(layer)
        project_down(layer)
        scatter(layer)
        norm_out(layer)

    weights_sent()
    down_sent()
    for layer in range(LAYERS):
        home_sent(layer)
        for t in range(3):
            for i in range(3):
                for k in (1, 2, 3):
                    gather_copy(layer, t, i, k, False).wait_send()
                    scatter_copy(layer, t, i, k, False).wait_send()


def on_device(tokens, pre_gain, post_gain, gate_weight, up_weight, down_weight):
    vmem = pl.BlockSpec(memory_space=pltpu.VMEM)
    hbm = pl.BlockSpec(memory_space=pl.ANY)
    dma = pltpu.SemaphoreType.DMA
    landing = []
    for t in range(3):
        order = ORDER[t][::-1]
        for i in range(3):
            landing.append(pltpu.VMEM((LAYERS, 3, *slab_shape(order[i], order[i + 1:]), 8, THIRD), BF16))
    return pl.pallas_call(
        kernel,
        out_shape=jax.ShapeDtypeStruct(tokens.shape, BF16),
        in_specs=[vmem, vmem, vmem, hbm, hbm, hbm],
        out_specs=vmem,
        scratch_shapes=[
            pltpu.VMEM((LAYERS, 2, SOURCES, ROWS, WIDE), BF16),
            pltpu.VMEM((LAYERS, WIDE, D), BF16),
            pltpu.VMEM((LAYERS, 3, 2, 4, 4, 2, 8, THIRD), BF16),
            pltpu.VMEM((LAYERS, 3, 2, 4, 4, 2, 8, THIRD), BF16),
            pltpu.VMEM((2, TOKENS, WIDE), F32),
            pltpu.VMEM((TOKENS, HALF), BF16),
            pltpu.VMEM((2, PART * ROWS, WIDE), BF16),
            pltpu.VMEM((256, WIDE), BF16),
            pltpu.VMEM((LAYERS, 3, 8, THIRD), BF16),
            pltpu.VMEM((LAYERS, 2, 256, WIDE), BF16),
            pltpu.VMEM((LAYERS, 2, 256, WIDE), BF16),
            pltpu.VMEM((2 * LAYERS, 8, 128), F32),
            pltpu.VMEM((2 * LAYERS, 8, 128), F32),
            pltpu.VMEM((8, HALF), F32),
            pltpu.VMEM((8, HALF), F32),
            *landing,
            dma((1,)), dma((LAYERS, PARTS)), dma((1,)), dma((LAYERS,)), dma((LAYERS,)), dma((LAYERS,)),
            dma((LAYERS, 3, 3, 3)), dma((LAYERS, 3, 3, 3)), dma((LAYERS, 3, 3, 3)), dma((LAYERS, 3, 3, 3)),
            dma((LAYERS,)), dma((LAYERS,)), dma((2 * LAYERS,)), dma((2 * LAYERS,)),
        ],
        compiler_params=pltpu.CompilerParams(has_side_effects=True, vmem_limit_bytes=67043328),
    )(tokens, pre_gain, post_gain, gate_weight, up_weight, down_weight)


def solution(mesh):
    weights = P(None, ("row", "col"), None)
    return jax.shard_map(
        on_device,
        mesh=mesh,
        in_specs=(P("col", "row"), P(None, "row"), P(None, "row"), weights, weights, weights),
        out_specs=P("col", "row"),
        check_vma=False,
    )
```
